32 devices in a mesh: expert: 16 (over z, y, core), dp: 2 (over x).
Axes of the slice: x: 2, y: 2, z: 4, core: 2. Of those that a mesh axis runs over, the one named last changes fastest.
Arguments:
- tokens: bfloat16 [4096, 2880], P(('expert', 'dp')), may hold values from -6 to 6
- cotangent: bfloat16 [4096, 2880], P(('expert', 'dp')), may hold values from -3 to 3
- expert_ids: int32 [4096, 4], P(('expert', 'dp')), may hold values from 0 to 15, as said below
- slots: int32 [4096, 4], P(('expert', 'dp')), may hold values from -1 to 23, as said below
- probs: float32 [4096, 4], P(('expert', 'dp')), may hold values from 0.1 to 0.6
- w_gate: bfloat16 [16, 2880, 1440], P('expert', None, 'dp'), may hold values from -0.109375 to 0.109375
- w_up: bfloat16 [16, 2880, 1440], P('expert', None, 'dp'), may hold values from -0.109375 to 0.109375
- w_down: bfloat16 [16, 2880, 1440], P('expert', None, 'dp'), may hold values from -0.15625 to 0.15625
Outputs:
- input_grad: bfloat16 [4096, 2880], P(('expert', 'dp'))
- prob_grad: float32 [4096, 4], P(('expert', 'dp'))
- grad_gate: bfloat16 [16, 2880, 1440], P('expert', None, 'dp')
- grad_up: bfloat16 [16, 2880, 1440], P('expert', None, 'dp')
- grad_down: bfloat16 [16, 2880, 1440], P('expert', None, 'dp')
The draws below stay inside these ranges and needn't reach their ends.
Inputs may be any that keep to these rules, and one draw needn't show every extreme that they name: `expert_ids`: each row names 4 different experts. Within the 128 tokens of one device, the choices of one expert, taken in order of tokens and then of k, hold 0, 1, 2 and so on up to 23, and -1 after that; in every draw some expert fills all 24 slots from every device.
All inputs are finite; a program needn't handle non-finite values.
Results may differ from the reference program's by a relative error of at most 0.018.
Values may be sent and summed in bfloat16 or wider, within the bound.
A program may use at most 192 MiB of HBM per device.

```python
import jax
import jax.numpy as jnp
from jax import lax

D = 2880
FFW = 1440
TOP = 4
TOK_DEV = 128
EXPERTS = 16
CAP = 24
TOKENS = 4096
N_EXPERT = 16
N_DP = 2


def routing_pair(key):
    base = jax.random.fold_in(key, 11)
    first_key, second_key, third_key = jax.random.split(base, 3)
    tokens_total = TOK_DEV * N_EXPERT * N_DP
    bias = jax.random.randint(first_key, (EXPERTS,), 0, 8192)
    hottest = jax.random.randint(second_key, (), 0, EXPERTS)
    expert_range = jnp.arange(EXPERTS, dtype=jnp.int32)
    bias = bias + jnp.where(expert_range == hottest, 40000, 0)
    scores = jax.random.randint(third_key, (tokens_total, EXPERTS), 0, 65536) + bias[None, :]
    scores = scores * EXPERTS + expert_range[None, :]
    ignored, chosen = lax.top_k(scores, TOP)
    chosen = chosen.astype(jnp.int32)
    onehot = (chosen[:, :, None] == expert_range[None, None, :]).astype(jnp.int32)
    onehot = onehot.reshape(tokens_total // TOK_DEV, TOK_DEV * TOP, EXPERTS)
    ranks = jnp.cumsum(onehot, axis=1) - 1
    ranks = jnp.sum(onehot * ranks, axis=2).reshape(tokens_total, TOP)
    slot_values = jnp.where(ranks < CAP, ranks, -1).astype(jnp.int32)
    return (chosen, slot_values)


def draw_expert_ids(key, part):
    chosen, slot_values = routing_pair(key)
    return chosen


def draw_slots(key, part):
    chosen, slot_values = routing_pair(key)
    return slot_values


def block_levels(stream_key, extent, cuts, low, top_value):
    loudness, own = 1.0, jax.random.fold_in(stream_key, 6)
    for dim, parts in cuts:
        steps = jnp.exp(jax.random.uniform(jax.random.fold_in(own, dim), (parts,), jnp.float32, low / len(cuts), top_value / len(cuts)))
        loudness = loudness * jnp.repeat(steps, extent[dim] // parts).reshape([-1 if axis == dim else 1 for axis in range(len(extent))])
    return loudness


def noise(rng, shape, width, most, cuts=(), held_as=jnp.bfloat16):
    drawn = width * jax.random.normal(rng, shape, jnp.float32)
    if cuts:
        drawn = drawn * block_levels(rng, shape, cuts, -0.22, 0.18)
    return jnp.clip(drawn, -most, most).astype(held_as)


def setup_inputs(seed: int = 0) -> dict:
    streams_of = jax.random.split(jax.random.key(seed), 9)
    return {
        "tokens": noise(streams_of[0], (TOKENS, D), 1.0, 6.0, ((0, 32),)),
        "cotangent": noise(streams_of[1], (TOKENS, D), 0.4, 3.0, ((0, 32),)),
        "expert_ids": draw_expert_ids(jax.random.fold_in(streams_of[8], 71), 0),
        "slots": draw_slots(jax.random.fold_in(streams_of[8], 71), 0),
        "probs": jnp.clip(0.1 + 0.5 * jax.random.uniform(streams_of[4], (TOKENS, TOP), jnp.float32) ** block_levels(streams_of[4], (TOKENS, TOP), ((0, 32),), -0.2, 0.2), 0.1, 0.6),
        "w_gate": noise(streams_of[5], (EXPERTS, D, FFW), D ** -0.5, 0.109375, ((0, 16), (2, 2))),
        "w_up": noise(streams_of[6], (EXPERTS, D, FFW), D ** -0.5, 0.109375, ((0, 16), (2, 2))),
        "w_down": noise(streams_of[7], (EXPERTS, D, FFW), FFW ** -0.5, 0.15625, ((0, 16), (2, 2))),
    }


ALPHA = 1.702


def reference(tokens, cotangent, expert_ids, slots, probs, w_gate, w_up, w_down):
    tokens_total = tokens.shape[0]
    blocks = tokens_total // TOK_DEV
    block_of = jnp.arange(tokens_total, dtype=jnp.int32) // TOK_DEV
    kept = slots >= 0
    position = jnp.where(kept, (expert_ids * blocks + block_of[:, None]) * CAP + slots, EXPERTS * blocks * CAP)
    owners = jnp.broadcast_to(jnp.arange(tokens_total, dtype=jnp.int32)[:, None], expert_ids.shape)
    slot_owner = jnp.full((EXPERTS * blocks * CAP,), -1, jnp.int32).at[position.reshape(-1)].set(owners.reshape(-1), mode="drop")
    slot_prob = jnp.zeros((EXPERTS * blocks * CAP,), jnp.float32).at[position.reshape(-1)].set(probs.reshape(-1), mode="drop")
    slot_owner = slot_owner.reshape(EXPERTS, blocks * CAP)
    slot_prob = slot_prob.reshape(EXPERTS, blocks * CAP)

    def expert_pass(operands):
        owner_col, prob_col, gate_w, up_w, down_w = operands
        present = owner_col >= 0
        source = jnp.maximum(owner_col, 0)
        rows = jnp.where(present[:, None], tokens[source], jnp.zeros((), jnp.bfloat16))
        gate_pre = jnp.dot(rows, gate_w, preferred_element_type=jnp.float32)
        up_pre = jnp.dot(rows, up_w, preferred_element_type=jnp.float32)
        sigmoid_val = jax.nn.sigmoid(ALPHA * gate_pre)
        glu_value = gate_pre * sigmoid_val
        hidden = ((up_pre + 1.0) * glu_value).astype(jnp.bfloat16)
        outputs = lax.dot_general(hidden, down_w, (((1,), (1,)), ((), ())), preferred_element_type=jnp.float32).astype(jnp.bfloat16)
        plain = jnp.where(present[:, None], cotangent[source], jnp.zeros((), jnp.bfloat16))
        slot_grad = jnp.sum(plain.astype(jnp.float32) * outputs.astype(jnp.float32), axis=1)
        weighted = (prob_col[:, None] * plain.astype(jnp.float32)).astype(jnp.bfloat16)
        hidden_grad = jnp.dot(weighted, down_w, preferred_element_type=jnp.float32)
        up_grad = (hidden_grad * glu_value).astype(jnp.bfloat16)
        gate_grad = (hidden_grad * (up_pre + 1.0) * (sigmoid_val + ALPHA * gate_pre * sigmoid_val * (1.0 - sigmoid_val))).astype(jnp.bfloat16)
        contract_rows = (((0,), (0,)), ((), ()))
        grad_down = lax.dot_general(weighted, hidden, contract_rows, preferred_element_type=jnp.float32).astype(jnp.bfloat16)
        grad_gate = lax.dot_general(rows, gate_grad, contract_rows, preferred_element_type=jnp.float32).astype(jnp.bfloat16)
        grad_up = lax.dot_general(rows, up_grad, contract_rows, preferred_element_type=jnp.float32).astype(jnp.bfloat16)
        contract_units = (((1,), (1,)), ((), ()))
        row_grad = lax.dot_general(gate_grad, gate_w, contract_units, preferred_element_type=jnp.float32)
        row_grad = row_grad + lax.dot_general(up_grad, up_w, contract_units, preferred_element_type=jnp.float32)
        return slot_grad, row_grad.astype(jnp.bfloat16), grad_gate, grad_up, grad_down

    slot_grads, row_grads, grad_gate, grad_up, grad_down = lax.map(expert_pass, (slot_owner, slot_prob, w_gate, w_up, w_down))
    lookup = jnp.where(kept, (expert_ids * blocks + block_of[:, None]) * CAP + slots, 0)
    prob_grad = jnp.where(kept, slot_grads.reshape(-1)[lookup], jnp.float32(0.0))
    flat_rows = row_grads.reshape(-1, tokens.shape[1])
    total = jnp.zeros(tokens.shape, jnp.float32)
    for choice_index in range(TOP):
        picked = flat_rows[lookup[:, choice_index]].astype(jnp.float32)
        total = total + jnp.where(kept[:, choice_index][:, None], picked, jnp.float32(0.0))
    input_grad = total.astype(jnp.bfloat16)
    return input_grad, prob_grad, grad_gate, grad_up, grad_down
```

```python
import functools

import jax
import jax.numpy as jnp
from jax import lax
from jax.experimental import pallas as pl
from jax.experimental.pallas import tpu as pltpu
from jax.sharding import PartitionSpec as P

ALPHA = 1.702
MESH = pl.DeviceIdType.MESH
ANY = pl.BlockSpec(memory_space=pl.ANY)


def offsets_of(count):
    half = count // 2
    order = []
    for step in range(half):
        order.append(half + step)
        if step:
            order.append(step)
    return order


def dispatch_kernel(count, tok_ref, cot_ref, rows_ref, wrows_ref, local_sem, send_sem, recv_sem, pass_sem, got_sem):
    me = lax.axis_index("expert")
    batch = lax.axis_index("dp")
    order = offsets_of(count)
    sources = (tok_ref, cot_ref)
    targets = (rows_ref, wrows_ref)

    def out_copy(a, o):
        peer = me ^ o
        return pltpu.make_async_remote_copy(
            src_ref=sources[a].at[peer],
            dst_ref=targets[a].at[batch, me],
            send_sem=send_sem.at[a, o],
            recv_sem=recv_sem.at[a, o],
            device_id=(peer, batch),
            device_id_type=MESH,
        )

    def in_copy(a, o):
        peer = me ^ o
        return pltpu.make_async_remote_copy(
            src_ref=sources[a].at[peer],
            dst_ref=targets[a].at[batch, peer],
            send_sem=send_sem.at[a, o],
            recv_sem=recv_sem.at[a, o],
            device_id=(peer, batch),
            device_id_type=MESH,
        )

    def pass_copy(a, o):
        peer = me ^ o
        src = targets[a].at[batch, peer] if o else sources[a].at[me]
        return pltpu.make_async_remote_copy(
            src_ref=src,
            dst_ref=targets[a].at[batch, peer],
            send_sem=pass_sem.at[a, o],
            recv_sem=got_sem.at[a, o],
            device_id=(me, 1 - batch),
            device_id_type=MESH,
        )

    def got_copy(a, o):
        peer = me ^ o
        return pltpu.make_async_remote_copy(
            src_ref=sources[a].at[peer],
            dst_ref=targets[a].at[1 - batch, peer],
            send_sem=pass_sem.at[a, o],
            recv_sem=got_sem.at[a, o],
            device_id=(me, 1 - batch),
            device_id_type=MESH,
        )

    def own_copy(a):
        return pltpu.make_async_copy(sources[a].at[me], targets[a].at[batch, me], local_sem.at[a])

    for o in order:
        out_copy(0, o).start()
    pass_copy(0, 0).start()
    own_copy(0).start()
    for o in order:
        in_copy(0, o).wait_recv()
        pass_copy(0, o).start()
        out_copy(1, o).start()
    pass_copy(1, 0).start()
    own_copy(1).start()
    for o in order:
        in_copy(1, o).wait_recv()
        pass_copy(1, o).start()
    for a in range(2):
        own_copy(a).wait()
        for o in order:
            out_copy(a, o).wait_send()
        for o in [0] + order:
            pass_copy(a, o).wait_send()
            got_copy(a, o).wait_recv()


def return_kernel(
    count, part_ref, dots_ref, back_ref, dback_ref, mine, got, total, load_sem, pass_sem, got_sem, send_sem, recv_sem, own_sem, dsend_sem, drecv_sem
):
    me = lax.axis_index("expert")
    batch = lax.axis_index("dp")
    order = offsets_of(count)

    def load_copy(o):
        peer = me ^ o
        return pltpu.make_async_copy(part_ref.at[batch, peer], mine.at[o], load_sem.at[o])

    def pass_copy(o):
        return pltpu.make_async_remote_copy(
            src_ref=part_ref.at[1 - batch, me ^ o],
            dst_ref=got.at[o],
            send_sem=pass_sem.at[o],
            recv_sem=got_sem.at[o],
            device_id=(me, 1 - batch),
            device_id_type=MESH,
        )

    def back_copy(o, slot):
        peer = me ^ o
        return pltpu.make_async_remote_copy(
            src_ref=total.at[o],
            dst_ref=back_ref.at[slot],
            send_sem=send_sem.at[o],
            recv_sem=recv_sem.at[o],
            device_id=(peer, batch),
            device_id_type=MESH,
        )

    def dot_copy(o, flip, slot_batch, slot):
        peer = me ^ o
        other = 1 - batch if flip else batch
        return pltpu.make_async_remote_copy(
            src_ref=dots_ref.at[other, peer],
            dst_ref=dback_ref.at[slot_batch, slot],
            send_sem=dsend_sem.at[flip, o],
            recv_sem=drecv_sem.at[flip, o],
            device_id=(peer, other),
            device_id_type=MESH,
        )

    def own_dots():
        return pltpu.make_async_copy(dots_ref.at[batch, me], dback_ref.at[batch, me], own_sem.at[1])

    def own_back():
        return pltpu.make_async_copy(total.at[0], back_ref.at[me], own_sem.at[0])

    for o in order + [0]:
        pass_copy(o).start()
        load_copy(o).start()
    own_dots().start()
    for o in [0] + order:
        for flip in range(2):
            if o or flip:
                dot_copy(o, flip, batch, me).start()
    for o in order + [0]:
        load_copy(o).wait()
        pass_copy(o).wait_recv()
        total[o] = (mine[o].astype(jnp.float32) + got[o].astype(jnp.float32)).astype(total.dtype)
        if o:
            back_copy(o, me).start()
        else:
            own_back().start()
    own_back().wait()
    own_dots().wait()
    for o in [0] + order:
        pass_copy(o).wait_send()
        if o:
            back_copy(o, me).wait_send()
            back_copy(o, me ^ o).wait_recv()
        for flip in range(2):
            if o or flip:
                dot_copy(o, flip, batch, me).wait_send()
                dot_copy(o, flip, 1 - batch if flip else batch, me ^ o).wait_recv()


def dispatch(tok_out, cot_out):
    count = tok_out.shape[0]
    shape = jax.ShapeDtypeStruct((2,) + tok_out.shape, tok_out.dtype)
    sems = pltpu.SemaphoreType.DMA((2, count))
    return pl.pallas_call(
        functools.partial(dispatch_kernel, count),
        out_shape=(shape, shape),
        in_specs=[ANY, ANY],
        out_specs=(ANY, ANY),
        scratch_shapes=[pltpu.SemaphoreType.DMA((2,)), sems, sems, sems, sems],
        compiler_params=pltpu.CompilerParams(has_side_effects=True, vmem_limit_bytes=4 * 2**20),
        name="dispatch",
    )(tok_out, cot_out)


def send_back(partial, dots):
    count = partial.shape[1]
    sems = pltpu.SemaphoreType.DMA((count,))
    pair_sems = pltpu.SemaphoreType.DMA((2, count))
    buffer = pltpu.VMEM(partial.shape[1:], partial.dtype)
    return pl.pallas_call(
        functools.partial(return_kernel, count),
        out_shape=(
            jax.ShapeDtypeStruct(partial.shape[1:], partial.dtype),
            jax.ShapeDtypeStruct(dots.shape, dots.dtype),
        ),
        in_specs=[ANY, ANY],
        out_specs=(ANY, ANY),
        scratch_shapes=[buffer, buffer, buffer, sems, sems, sems, sems, sems, pltpu.SemaphoreType.DMA((2,)), pair_sems, pair_sems],
        compiler_params=pltpu.CompilerParams(has_side_effects=True, vmem_limit_bytes=32 * 2**20),
        name="send_back",
    )(partial, dots)


def body(tokens, cotangent, expert_ids, slots, probs, w_gate, w_up, w_down):
    experts = lax.axis_size("expert")
    tok_rows, width = tokens.shape
    top_count = expert_ids.shape[1]
    capacity = max(2, 3 * tok_rows * top_count // (4 * experts))
    slot_total = experts * capacity
    kept = slots >= 0
    position = jnp.where(kept, expert_ids * capacity + slots, -1)
    slot_range = jnp.arange(slot_total, dtype=jnp.int32)
    hits = position.T[:, :, None] == slot_range[None, None, :]
    hot = jnp.any(hits, axis=0).astype(jnp.bfloat16)
    contract_first = (((0,), (0,)), ((), ()))
    slot_prob = jnp.sum(jnp.where(hits, probs.T[:, :, None], jnp.float32(0.0)), axis=(0, 1))
    tok_out = lax.dot_general(hot, tokens, contract_first, preferred_element_type=jnp.float32).astype(jnp.bfloat16)
    cot_out = (
        slot_prob[:, None] * lax.dot_general(hot, cotangent, contract_first, preferred_element_type=jnp.float32)
    ).astype(jnp.bfloat16)
    rows, wrows = dispatch(
        tok_out.reshape(experts, capacity, width), cot_out.reshape(experts, capacity, width)
    )
    pair_rows = rows.reshape(2 * slot_total, width)
    pair_cot = wrows.reshape(2 * slot_total, width)
    gate_w = w_gate[0]
    up_w = w_up[0]
    down_w = w_down[0]
    gate_pre = jnp.dot(pair_rows, gate_w, preferred_element_type=jnp.float32)
    up_pre = jnp.dot(pair_rows, up_w, preferred_element_type=jnp.float32)
    sigmoid_val = jax.nn.sigmoid(ALPHA * gate_pre)
    glu_value = gate_pre * sigmoid_val
    hidden = ((up_pre + 1.0) * glu_value).astype(jnp.bfloat16)
    contract_units = (((1,), (1,)), ((), ()))
    hidden_grad = jnp.dot(pair_cot, down_w, preferred_element_type=jnp.float32)
    dots = jnp.sum(hidden_grad * hidden.astype(jnp.float32), axis=1)
    up_grad = (hidden_grad * glu_value).astype(jnp.bfloat16)
    gate_grad = (
        hidden_grad
        * (up_pre + 1.0)
        * (sigmoid_val + ALPHA * gate_pre * sigmoid_val * (1.0 - sigmoid_val))
    ).astype(jnp.bfloat16)
    partial = (
        lax.dot_general(gate_grad, gate_w, contract_units, preferred_element_type=jnp.float32)
        + lax.dot_general(up_grad, up_w, contract_units, preferred_element_type=jnp.float32)
    ).astype(jnp.bfloat16)
    lanes = -(-capacity // 128) * 128
    dots = jnp.pad(dots.reshape(2, experts, 1, capacity), ((0, 0), (0, 0), (0, 0), (0, lanes - capacity)))
    back, dots_back = send_back(partial.reshape(2, experts, capacity, width), dots)
    grad_down = lax.dot_general(
        pair_cot, hidden, contract_first, preferred_element_type=jnp.float32
    ).astype(jnp.bfloat16)
    grad_gate = lax.dot_general(
        pair_rows, gate_grad, contract_first, preferred_element_type=jnp.float32
    ).astype(jnp.bfloat16)
    grad_up = lax.dot_general(
        pair_rows, up_grad, contract_first, preferred_element_type=jnp.float32
    ).astype(jnp.bfloat16)
    slot_dots = jnp.sum(dots_back[:, :, 0, :capacity], axis=0).reshape(slot_total)
    inner = jnp.sum(jnp.where(hits, slot_dots[None, None, :], jnp.float32(0.0)), axis=2).T
    prob_grad = jnp.where(kept, inner / probs, jnp.float32(0.0))
    input_grad = jnp.dot(
        hot, back.reshape(slot_total, width), preferred_element_type=jnp.float32
    ).astype(jnp.bfloat16)
    return (input_grad, prob_grad, grad_gate[None], grad_up[None], grad_down[None])


def solution(mesh):
    return jax.shard_map(
        body,
        mesh=mesh,
        in_specs=(
            P(("expert", "dp"), None),
            P(("expert", "dp"), None),
            P(("expert", "dp"), None),
            P(("expert", "dp"), None),
            P(("expert", "dp"), None),
            P("expert", None, "dp"),
            P("expert", None, "dp"),
            P("expert", None, "dp"),
        ),
        out_specs=(
            P(("expert", "dp"), None),
            P(("expert", "dp"), None),
            P("expert", None, "dp"),
            P("expert", None, "dp"),
            P("expert", None, "dp"),
        ),
        check_vma=False,
    )
```
